256 devices in a mesh: replica: 16 (over z_hi, x), shard: 16 (over y, z_lo, core).
Axes of the slice: x: 4, y: 4, z: 8 (z_hi: 4, z_lo: 2; z = z_hi * 2 + z_lo), core: 2. Of those that a mesh axis runs over, the one named last changes fastest.
Arguments:
- deltas: bfloat16 [16, 8192, 8192], P('replica', 'shard')
- master: float32 [8192, 8192], P('shard', 'replica'), may hold values from -6 to 6
- momentum: float32 [8192, 8192], P('shard', 'replica'), may hold values from -6 to 6
- block_owner: int32 [32, 1], replicated, may hold values from 0 to 15; in each aligned block of 32 rows (0 to 31, 32 to 63, ...) at most 4 rows name the same one
Outputs:
- master_out: float32 [8192, 8192], P('shard', 'replica')
- momentum_out: float32 [8192, 8192], P('shard', 'replica')
- params: bfloat16 [4096, 8192], P(None, 'replica')
The draws below stay inside these ranges and needn't reach their ends.
Inputs may be any that keep to these rules, and one draw needn't show every extreme that they name: `block_owner`: every shard owns at least one block and at most 4; some shard owns exactly 4. Rows of slots that are not live hold arbitrary deltas.
All inputs are finite; a program needn't handle non-finite values.
Results may differ from the reference program's by a relative error of at most 0.01.
Values may be sent and summed in bfloat16 or wider, within the bound.
No kernel may reach another device: no remote copies, remote signals or barrier semaphores. Data moves between devices by JAX's collectives and lax.ppermute only.
A program may use at most 128 MiB of HBM per device.

```python
import math
import jax
import jax.numpy as jnp
import numpy as np
from jax import lax

D = 8192
BLOCK_ROWS = 128
SLOTS = 4
BLOCKS = 32
N_REPLICA = 16
N_SHARD = 16


def draw_deltas(key, part):
    rows = N_SHARD * SLOTS * BLOCK_ROWS
    base = jax.random.normal(key, (N_REPLICA, rows, D), jnp.float32)
    ramp = jnp.exp(jnp.log(3.0) * jnp.arange(rows, dtype=jnp.float32) / max(rows - 1, 1))
    rising = jnp.exp(jnp.log(3.0) * jnp.arange(N_REPLICA, dtype=jnp.float32) / max(N_REPLICA - 1, 1))
    column_ramp = jnp.exp(jnp.log(3.0) * jnp.arange(D, dtype=jnp.float32) / max(D - 1, 1))
    values = base * column_ramp[None, None, :]
    return (4.0 * values * ramp[None, :, None] * rising[:, None, None]).astype(jnp.bfloat16)


def levels(key, shape, cuts, smallest, largest):
    level, own = 1.0, jax.random.fold_in(key, 6)
    for dim, blocks in cuts:
        draws = jnp.exp(jax.random.uniform(jax.random.fold_in(own, dim), (blocks,), jnp.float32, smallest / len(cuts), largest / len(cuts)))
        level = level * jnp.repeat(draws, shape[dim] // blocks).reshape([-1 if axis == dim else 1 for axis in range(len(shape))])
    return level


def shared_out(own_key, own, number, rows, count, top, reach, slope):
    sequence = jax.random.permutation(own_key, count)
    packed, usual = load_shares(count, rows * top, reach, slope, True), load_shares(count, rows * top, reach, slope, False)
    places = jnp.arange(count)

    def named(lengths, offset_by):
        used = int((lengths > 0).sum())
        fixed = max(1, used // 4)
        moved = fixed + (places - fixed + offset_by * (used - fixed)) % max(1, count - fixed)
        return jnp.zeros((count,), jnp.int32).at[sequence[jnp.where(places < fixed, places, moved)]].set(jnp.asarray(lengths, jnp.int32))

    lengths = jnp.where(number % 4 == 0, named(packed, number // 4), named(usual, number - number // 4 - 1))
    mixed = jax.random.permutation(jax.random.fold_in(own, 3), count)
    giver, sink = mixed[0:count // 2 * 2:2], mixed[1:count // 2 * 2:2]
    slack = jnp.minimum(lengths[giver] - 1, reach - lengths[sink]) // 2
    slack = jnp.where((giver == sequence[0]) | (sink == sequence[0]) | (lengths[sink] == 0), 0, jnp.maximum(slack, 0))
    moved = jax.random.randint(jax.random.fold_in(own, 4), (count // 2,), 0, 1 << 20) % (slack + 1)
    lengths = lengths.at[giver].add(-moved).at[sink].add(moved)
    items = jnp.searchsorted(jnp.cumsum(lengths), jnp.arange(rows * top), side="right").astype(jnp.int32)
    table = items.reshape(top, rows).T
    table = table[jax.random.permutation(jax.random.fold_in(own, 1), rows)]
    offset_by = jax.random.randint(jax.random.fold_in(own, 2), (rows, 1), 0, top)
    return jnp.take_along_axis(table, (jnp.arange(top)[None, :] + offset_by) % top, axis=1)


def load_shares(number_of, total, reach, skew, full):
    loads = [(1 << 20) // math.isqrt(grade ** skew) + 1 for grade in range(1, number_of + 1)]
    largest = reach if full else min(reach, max(-(-total // number_of), total * loads[0] // sum(loads)))
    least = 1 if total - largest >= number_of - 1 else 0
    given, spare = [largest] + [least] * (number_of - 1), total - largest - least * (number_of - 1)
    while spare > 0:
        candidates = [i for i in range(1, number_of) if given[i] < largest] or [i for i in range(1, number_of) if given[i] < reach]
        whole, left = sum([loads[i] for i in candidates]), spare
        for i in candidates:
            more = min(reach - given[i], max(1, left * loads[i] // whole), spare)
            given[i] = given[i] + more
            spare = spare - more
    return np.array(given)


def normal_values(key, extent, deviation, most, cuts=(), held_as=jnp.bfloat16):
    gain = levels(key, extent, cuts, -0.22, 0.18) if cuts else 1.0
    result = jax.random.normal(key, extent, jnp.float32) * deviation * gain
    return jnp.minimum(jnp.maximum(result, -most), most).astype(held_as)


def setup_inputs(seed: int = 0) -> dict:
    arg_keys = jax.random.split(jax.random.key(seed), 5)
    deltas = draw_deltas(jax.random.fold_in(arg_keys[4], 71), 0)
    master = normal_values(arg_keys[1], (N_SHARD * SLOTS * BLOCK_ROWS, D), 1.0, 6.0, ((0, 16), (1, 16)), jnp.float32)
    momentum = normal_values(arg_keys[2], (N_SHARD * SLOTS * BLOCK_ROWS, D), 1.0, 6.0, ((0, 16), (1, 16)), jnp.float32)
    block_owner_keys = jax.random.split(jax.random.fold_in(arg_keys[3], 1), BLOCKS // BLOCKS)
    block_owner_turns = jax.random.permutation(jax.random.fold_in(arg_keys[3], 3), BLOCKS // BLOCKS)
    block_owner = jax.vmap(lambda own, number: shared_out(jax.random.fold_in(arg_keys[3], 2), own, number, BLOCKS, N_SHARD, 1, SLOTS, 2))(block_owner_keys, block_owner_turns).reshape((BLOCKS, 1))
    return dict(deltas=deltas, master=master, momentum=momentum, block_owner=block_owner)


def reference(deltas, master, momentum, block_owner):
    owner = block_owner[:, 0]
    shard_ids = jnp.arange(N_SHARD, dtype=jnp.int32)
    counts = lax.optimization_barrier(jnp.sum((owner[None, :] == shard_ids[:, None]).astype(jnp.int32), axis=1))
    live = jnp.arange(SLOTS, dtype=jnp.int32)[None, :] < counts[:, None]
    live_rows = jnp.repeat(live.reshape(-1), BLOCK_ROWS)[:, None]

    def add_one(total, piece):
        return (total + piece.astype(jnp.float32), None)
    summed, _ = lax.scan(add_one, jnp.zeros(master.shape, jnp.float32), deltas)
    avg = jnp.where(live_rows, summed / N_REPLICA, jnp.float32(0.0))
    total = jnp.sum(avg * avg)
    limit = 0.5 * jnp.sqrt(jnp.float32(BLOCKS * BLOCK_ROWS * D))
    factor = jnp.minimum(jnp.float32(1.0), limit / (jnp.sqrt(total) + 1e-06))
    grad = factor * avg
    momentum_out = jnp.where(live_rows, 0.9 * momentum + grad, momentum)
    master_out = jnp.where(live_rows, master - 0.7 * (grad + 0.9 * momentum_out), master)
    index = jnp.arange(BLOCKS, dtype=jnp.int32)
    same = (owner[None, :] == owner[:, None]) & (index[None, :] < index[:, None])
    before = lax.optimization_barrier(jnp.sum(same.astype(jnp.int32), axis=1))
    flat = (owner * SLOTS + before).astype(jnp.int32)
    blocks = master_out.reshape(N_SHARD * SLOTS, BLOCK_ROWS, D)[flat]
    params = blocks.astype(jnp.bfloat16).reshape(BLOCKS * BLOCK_ROWS, D)
    return (master_out, momentum_out, params)
```

```python
import functools

import jax
import jax.numpy as jnp
from jax import lax
from jax.experimental import pallas as pl
from jax.experimental.pallas import tpu as pltpu
from jax.sharding import Mesh
from jax.sharding import PartitionSpec as P

BLOCK_ROWS = 128
SLOTS = 4
BLOCKS = 32
REPLICA = ("zh", "x")
SHARD = ("y", "zl", "c")
ALL = REPLICA + SHARD
BF = jnp.bfloat16
F = jnp.float32
W = 512


def perm(v, ax, d):
    n = lax.axis_size(ax)
    return lax.ppermute(v, ax, [(i, (i + d) % n) for i in range(n)])


def pos(s):
    return s[0] // 64, (s[0] // 16) % 4


def m4(v):
    return lax.rem(v + 8, 4)


def gsum(me, outs, shape):
    terms = [t for _, pieces in outs for piece in pieces for t in piece]
    counts = [[len(piece) for piece in pieces] for _, pieces in outs]

    def body(s, *refs):
        ins, os, token = refs[: len(terms)], refs[len(terms):-1], refs[-1]
        token[0] = s[0]
        k = 0
        for o, cs in zip(os, counts):
            for p, c in enumerate(cs):
                if c == 1:
                    o[p] = ins[k][...].reshape(shape).astype(o.dtype)
                else:
                    acc = ins[k][...].reshape(shape).astype(F)
                    for t in range(1, c):
                        acc = acc + ins[k + t][...].reshape(shape).astype(F)
                    o[p] = acc.astype(o.dtype)
                k += c

    def spec(t):
        _, block, imap = t
        return pl.BlockSpec(block, lambda i, s: imap(*pos(s)))

    results = pl.pallas_call(
        body,
        grid_spec=pltpu.PrefetchScalarGridSpec(
            num_scalar_prefetch=1,
            grid=(1,),
            in_specs=[spec(t) for t in terms],
            out_specs=[pl.BlockSpec((len(p),) + shape, lambda i, s: (0, 0, 0)) for _, p in outs]
            + [pl.BlockSpec(memory_space=pltpu.SMEM)],
        ),
        out_shape=[jax.ShapeDtypeStruct((len(p),) + shape, d) for d, p in outs]
        + [jax.ShapeDtypeStruct((1,), jnp.int32)],
    )(me, *[t[0] for t in terms])
    return results[:-1], results[-1]


class XDirect:
    first_axis, second_axis = "x", "zh"

    def __init__(self, D, r0, n):
        self.D, self.r0, self.n = D, r0, n

    def own(self, col, w=W):
        return (self.D, (pl.Element(self.n), pl.Element(w)), lambda zh, x: (self.r0, pl.multiple_of(col(zh, x) * w, w)))

    def pack(self, me):
        pieces = lambda o: [[self.own(lambda zh, x, z=z: z * 4 + m4(x + o))] for z in range(4)]
        return gsum(me, [(BF, pieces(o)) for o in (1, 2, 3)], (self.n, W))

    def first(self, sends):
        self.recv = [perm(s, self.first_axis, o) for s, o in zip(sends, (1, 2, 3))]

    def part(self, o):
        return [self.own(lambda zh, x: m4(zh + o) * 4 + x)] + [
            (r, (1, self.n, W), lambda zh, x: (m4(zh + o), 0, 0)) for r in self.recv
        ]

    def mid(self, me):
        return gsum(me, [(BF, [self.part(o)]) for o in (1, 2, 3)] + [(F, [self.part(0)])], (self.n, W))

    def second(self, pieces):
        self.keep = pieces[3]
        self.recv = [perm(s, self.second_axis, o) for s, o in zip(pieces, (1, 2, 3))]

    def final(self, me):
        a = lambda arr: (arr, (1, self.n, W), lambda zh, x: (0, 0, 0))
        (out,), me = gsum(me, [(F, [[a(self.keep)] + [a(r) for r in self.recv]])], (self.n, W))
        return out.reshape(self.n, W), me


class ZDirect(XDirect):
    first_axis, second_axis = "zh", "x"

    def pack(self, me):
        return gsum(me, [(BF, [[self.own(lambda zh, x, o=o: m4(zh + o), 4 * W)]]) for o in (1, 2, 3)], (self.n, 4 * W))

    def part(self, o):
        return [self.own(lambda zh, x: zh * 4 + m4(x + o))] + [
            (r, (1, self.n, W), lambda zh, x: (0, 0, m4(x + o))) for r in self.recv
        ]


def replica_sums(me, chunks, last):
    for c in chunks:
        sends, me = c.pack(me)
        c.first(sends)
    for c in chunks:
        sends, me = c.mid(me)
        c.second(sends)
    sums = {}
    for i in last:
        sums[i], me = chunks[i].final(me)
    return [sums[i] for i in range(len(chunks))]


def total_over(x):
    n = lax.axis_size(ALL)
    return jnp.sum(lax.all_to_all(jnp.broadcast_to(x, (n,)), ALL, 0, 0, tiled=True))


def pick(same, index, mine, partner):
    def body(same_ref, index_ref, mine_ref, partner_ref, out_ref, sems):
        for b in range(BLOCKS):
            i = index_ref[b]

            @pl.when(same_ref[b] == 1)
            def _():
                pltpu.make_async_copy(mine_ref.at[i], out_ref.at[b], sems.at[b]).start()

            @pl.when(same_ref[b] == 0)
            def _():
                pltpu.make_async_copy(partner_ref.at[i], out_ref.at[b], sems.at[b]).start()

        for b in range(BLOCKS):
            pltpu.make_async_copy(mine_ref.at[0], out_ref.at[b], sems.at[b]).wait()

    smem = pl.BlockSpec(memory_space=pltpu.SMEM)
    hbm = pl.BlockSpec(memory_space=pltpu.HBM)
    return pl.pallas_call(
        body,
        in_specs=[smem, smem, hbm, hbm],
        out_specs=pl.BlockSpec(memory_space=pltpu.VMEM),
        out_shape=jax.ShapeDtypeStruct((BLOCKS, BLOCK_ROWS, W), mine.dtype),
        scratch_shapes=[pltpu.SemaphoreType.DMA((BLOCKS,))],
    )(same, index, mine, partner)


def gather_columns(x):
    n = lax.axis_size(("y", "zl"))
    mine = lax.all_to_all(jnp.broadcast_to(x[None], (n,) + x.shape), ("y", "zl"), 0, 0, tiled=True)
    return mine, perm(mine, "c", 1)


def on_device(deltas, master, momentum, block_owner):
    replicas = lax.axis_size(REPLICA)
    me_shard = lax.axis_index(SHARD)
    me = lax.axis_index(ALL).reshape(1)
    D = deltas[0]
    width = D.shape[1]
    owner = block_owner[:, 0]
    mine_count = jnp.sum((owner == me_shard).astype(jnp.int32))
    live_rows = (lax.broadcasted_iota(jnp.int32, (SLOTS * BLOCK_ROWS, 1), 0) // BLOCK_ROWS) < mine_count

    chunks = [XDirect(D, 0, 208), ZDirect(D, 208, 96), XDirect(D, 304, 208)]
    summed = jnp.concatenate(replica_sums(me, chunks, (0, 1, 2)), axis=0)
    avg = jnp.where(live_rows, summed / replicas, F(0.0))
    total = total_over(jnp.sum(avg * avg))
    limit = 0.5 * jnp.sqrt(F(BLOCKS * BLOCK_ROWS * width))
    factor = jnp.minimum(F(1.0), limit / (jnp.sqrt(total) + 1e-06))
    grad = factor * avg
    momentum_out = jnp.where(live_rows, 0.9 * momentum + grad, momentum)
    master_out = jnp.where(live_rows, master - 0.7 * (grad + 0.9 * momentum_out), master)
    updated = master_out.astype(BF).reshape(SLOTS, BLOCK_ROWS, W)
    index = jnp.arange(BLOCKS, dtype=jnp.int32)
    same = (owner[None, :] == owner[:, None]) & (index[None, :] < index[:, None])
    before = jnp.sum(same.astype(jnp.int32), axis=1)
    mine, partner = gather_columns(updated)
    place = (owner // 2) * SLOTS + before
    same_core = (owner % 2 == me_shard % 2).astype(jnp.int32)
    blocks = pick(same_core, place, *(a.reshape(-1, BLOCK_ROWS, W) for a in (mine, partner)))
    params = blocks.reshape(BLOCKS * BLOCK_ROWS, W)
    return (master_out, momentum_out, params)


def solution(mesh):
    finer = Mesh(mesh.devices.reshape(4, 4, 4, 2, 2), ALL)
    in_specs = (P(REPLICA, SHARD, None), P(SHARD, REPLICA), P(SHARD, REPLICA), P())
    out_specs = (P(SHARD, REPLICA), P(SHARD, REPLICA), P(None, REPLICA))
    return jax.shard_map(
        on_device, mesh=finer, in_specs=in_specs, out_specs=out_specs, check_vma=False
    )
```
